256 devices in a mesh: shift: 4 (over x), fsdp: 32 (over z, y_lo, core), tp: 2 (over y_hi).
Axes of the slice: x: 4, y: 4 (y_hi: 2, y_lo: 2; y = y_hi * 2 + y_lo), z: 8, core: 2. Of those that a mesh axis runs over, the one named last changes fastest.
Arguments:
- grad_stack: float32 [512, 128, 2048], P('shift', 'fsdp', 'tp'), parts along dimension 0, may hold values from -6 to 6
- moment_stack: float32 [512, 128, 2048], P('shift', 'fsdp', 'tp'), parts along dimension 0, may hold values from -6 to 6
- weight_stack: float32 [512, 128, 2048], P('shift', 'fsdp', 'tp'), parts along dimension 0, may hold values from -0.1875 to 0.1875
Outputs:
- new_weights: float32 [512, 128, 2048], P('shift', 'fsdp', 'tp'), parts along dimension 0
- new_momentum: float32 [512, 128, 2048], P('shift', 'fsdp', 'tp'), parts along dimension 0
The draws below stay inside these ranges and needn't reach their ends.
There are 4 independent parts, one for each index of `shift`. The reference program is written for one: setup_inputs(seed, part) draws one part's arguments, and reference() takes and returns one part's arrays. A program takes and returns all parts, laid end to end along the dimension named above; each array names one. Nothing has to cross between parts.
All inputs are finite; a program needn't handle non-finite values.
Results may differ from the reference program's by a relative error of at most 0.0003.
Values sent between devices are 32-bit elements.
A program may use at most 64 MiB of HBM per device.

```python
import jax
import jax.numpy as jnp
from jax import lax

SIDE = 128
WIDE = 2048
MATS = 128
ITERS = 3


def block_scale(key, dims, cuts, smallest, largest):
    loudness, own = 1.0, jax.random.fold_in(key, 6)
    for position, parts in cuts:
        draws = jnp.exp(jax.random.uniform(jax.random.fold_in(own, position), (parts,), jnp.float32, smallest / len(cuts), largest / len(cuts)))
        loudness = loudness * jnp.repeat(draws, dims[position] // parts).reshape([-1 if axis == position else 1 for axis in range(len(dims))])
    return loudness


def gaussian(rng, shape, spread, reach, split=(), dtype=jnp.bfloat16):
    factor_of = block_scale(rng, shape, split, -0.22, 0.18) if split else 1.0
    array = jax.random.normal(rng, shape, jnp.float32) * spread * factor_of
    return jnp.minimum(jnp.maximum(array, -reach), reach).astype(dtype)


def setup_inputs(seed: int = 0, part: int = 0) -> dict:
    key_list = jax.random.split(jax.random.key(seed), 4)
    part_splits = jax.random.split(jax.random.fold_in(key_list[3], part), 4)
    grad_stack = gaussian(part_splits[0], (MATS, SIDE, WIDE), 1.0, 6.0, ((1, 32), (2, 2)), jnp.float32)
    moment_stack = gaussian(part_splits[1], (MATS, SIDE, WIDE), 1.0, 6.0, ((1, 32), (2, 2)), jnp.float32)
    weight_stack = gaussian(part_splits[2], (MATS, SIDE, WIDE), 0.03, 0.1875, ((1, 32), (2, 2)), jnp.float32)
    return dict(grad_stack=grad_stack, moment_stack=moment_stack, weight_stack=weight_stack)


hold_rate = 0.95
learn_rate = 0.9

def reference(grad_stack, moment_stack, weight_stack):
    new_momentum = hold_rate * moment_stack + grad_stack

    def orthogonal_one(stack):
        iterate = stack[None]
        iterate = iterate * lax.rsqrt(lax.optimization_barrier(jnp.sum(iterate * iterate, axis=(1, 2), keepdims=True)) + 1e-06)
        for step in range(ITERS):
            gram = jnp.einsum('mik,mjk->mij', iterate, iterate, precision=lax.Precision.HIGHEST)
            mixed = -4.775 * gram + 2.0315 * jnp.einsum('mij,mjk->mik', gram, gram, precision=lax.Precision.HIGHEST)
            iterate = 3.4445 * iterate + jnp.einsum('mij,mjk->mik', mixed, iterate, precision=lax.Precision.HIGHEST)
        return iterate[0]
    iterate = lax.map(orthogonal_one, new_momentum)
    new_weights = weight_stack - learn_rate * iterate
    return (new_weights, new_momentum)
```

```python
import functools

import jax
import jax.numpy as jnp
from jax import lax
from jax.experimental import pallas as pl
from jax.experimental.pallas import tpu as pltpu
from jax.sharding import PartitionSpec as P

MESH = pl.DeviceIdType.MESH
ITERS = 3
hold_rate = 0.95
learn_rate = 0.9


def full_dot(a, b, dims):
    return lax.dot_general(
        a, b, (dims, ((), ())), precision=lax.Precision.HIGHEST, preferred_element_type=jnp.float32
    )


def times(a, b):
    return full_dot(a, b, ((1,), (0,)))


def polynomial(gram):
    side = gram.shape[0]
    eye = lax.broadcasted_iota(jnp.int32, (side, side), 0) == lax.broadcasted_iota(
        jnp.int32, (side, side), 1
    )
    total = jnp.sum(jnp.sum(jnp.where(eye, gram, 0.0), axis=1, keepdims=True), axis=0, keepdims=True)
    scale = lax.rsqrt(total + 1e-06)
    a = gram * (scale * scale)
    whole = None
    for step in range(ITERS):
        mixed = -4.775 * a + 2.0315 * times(a, a)
        mixed = jnp.where(eye, mixed + 3.4445, mixed)
        whole = mixed if whole is None else times(mixed, whole)
        if step < ITERS - 1:
            a = times(times(mixed, a), mixed)
    return whole * scale


def kernel(
    group,
    waves,
    g_ref,
    m_ref,
    w_ref,
    weights,
    momentum,
    g_buf,
    m_buf,
    w_buf,
    arrived,
    leaving,
    returned,
    rows,
    gram_out,
    gram_in,
    load_sem,
    w_sem,
    out_send,
    out_recv,
    gram_send,
    gram_recv,
    back_send,
    back_recv,
):
    me, half = lax.axis_index("fsdp"), lax.axis_index("tp")
    near, other = rows.shape[0] // group, lax.rem(half + 1, 2)

    def peer(o):
        return lax.rem(me + o, group)

    barrier = pltpu.get_barrier_semaphore()

    def greet(o, _):
        pl.semaphore_signal(barrier, inc=1, device_id={"fsdp": peer(o)}, device_id_type=MESH)
        return 0

    lax.fori_loop(1, group, greet, 0)
    pl.semaphore_signal(barrier, inc=1, device_id={"tp": other}, device_id_type=MESH)

    def part(w):
        return pl.ds(w * group, group)

    def loads(w):
        return (
            pltpu.make_async_copy(g_ref.at[part(w)], g_buf.at[part(w)], load_sem.at[0, w]),
            pltpu.make_async_copy(m_ref.at[part(w)], m_buf.at[part(w)], load_sem.at[1, w]),
        )

    for w in range(waves):
        for copy in loads(w):
            copy.start()
    w_copy = pltpu.make_async_copy(w_ref, w_buf, w_sem)
    w_copy.start()

    def out_copy(w, o):
        return pltpu.make_async_remote_copy(
            src_ref=momentum.at[w * group + peer(o)],
            dst_ref=arrived.at[w, me],
            send_sem=out_send.at[w],
            recv_sem=out_recv.at[w],
            device_id={"fsdp": peer(o)},
            device_id_type=MESH,
        )

    def back_copy(w, o):
        return pltpu.make_async_remote_copy(
            src_ref=leaving.at[w, peer(o)],
            dst_ref=returned.at[w * group + me],
            send_sem=back_send.at[w],
            recv_sem=back_recv.at[w],
            device_id={"fsdp": peer(o)},
            device_id_type=MESH,
        )

    def all_of(buf, send, recv):
        return pltpu.make_async_remote_copy(
            src_ref=buf, dst_ref=buf, send_sem=send, recv_sem=recv,
            device_id={"fsdp": me}, device_id_type=MESH,
        )

    def gram_copy(w):
        return pltpu.make_async_remote_copy(
            src_ref=gram_out.at[w],
            dst_ref=gram_in.at[w],
            send_sem=gram_send.at[w],
            recv_sem=gram_recv.at[w],
            device_id={"tp": other},
            device_id_type=MESH,
        )

    for w in range(waves):
        for copy in loads(w):
            copy.wait()
        momentum[part(w)] = hold_rate * m_buf[part(w)] + g_buf[part(w)]
        if w == 0:
            pl.semaphore_wait(barrier, group)

        def send(o, _, w=w):
            out_copy(w, o).start()
            return 0

        lax.fori_loop(1, group, send, 0)
        arrived[w, me] = momentum[w * group + me]

    def wave(w, _):
        all_of(arrived.at[w, pl.ds(0, group - 1)], out_send.at[w], out_recv.at[w]).wait_recv()
        for k in range(group // 2):
            rows[pl.ds(2 * near * k, 2 * near), :] = jnp.concatenate(
                [arrived[w, 2 * k], arrived[w, 2 * k + 1]], axis=0
            )
        mat = rows[...]
        gram_out[w] = full_dot(mat, mat, ((1,), (1,)))
        gram_copy(w).start()
        gram_copy(w).wait_recv()
        mix = polynomial(gram_out[w] + gram_in[w])
        product = times(mix, rows[...])
        for k in range(group):
            leaving[w, k] = product[near * k : near * (k + 1)]

        def send(o, _):
            back_copy(w, o).start()
            return 0

        lax.fori_loop(1, group, send, 0)
        returned[w * group + me] = leaving[w, me]
        return 0

    lax.fori_loop(0, waves, wave, 0)
    w_copy.wait()

    def finish(w, _):
        all_of(returned.at[pl.ds(w * group, group - 1)], back_send.at[w], back_recv.at[w]).wait_recv()
        weights[part(w)] = w_buf[part(w)] - learn_rate * returned[part(w)]
        return 0

    lax.fori_loop(0, waves, finish, 0)

    def drain(w, _):
        all_of(arrived.at[w, pl.ds(0, group - 1)], out_send.at[w], out_recv.at[w]).wait_send()
        gram_copy(w).wait_send()
        all_of(returned.at[pl.ds(w * group, group - 1)], back_send.at[w], back_recv.at[w]).wait_send()
        return 0

    lax.fori_loop(0, waves, drain, 0)


def solution(mesh):
    group = mesh.shape["fsdp"]

    def body(g, m, w):
        mats, near, wide = g.shape
        waves, side = mats // group, near * group
        block = jax.ShapeDtypeStruct(g.shape, jnp.float32)
        f32 = jnp.float32
        sem = pltpu.SemaphoreType.DMA
        return pl.pallas_call(
            functools.partial(kernel, group, waves),
            name="update",
            out_shape=(block, block),
            in_specs=[pl.BlockSpec(memory_space=pltpu.HBM)] * 3,
            out_specs=[pl.BlockSpec(memory_space=pltpu.VMEM)] * 2,
            scratch_shapes=[
                pltpu.VMEM(g.shape, f32),
                pltpu.VMEM(g.shape, f32),
                pltpu.VMEM(g.shape, f32),
                pltpu.VMEM((waves, group, near, wide), f32),
                pltpu.VMEM((waves, group, near, wide), f32),
                pltpu.VMEM(g.shape, f32),
                pltpu.VMEM((side, wide), f32),
                pltpu.VMEM((waves, side, side), f32),
                pltpu.VMEM((waves, side, side), f32),
                sem((2, waves)),
                sem,
                sem((waves,)),
                sem((waves,)),
                sem((waves,)),
                sem((waves,)),
                sem((waves,)),
                sem((waves,)),
            ],
            compiler_params=pltpu.CompilerParams(
                collective_id=0, has_side_effects=True, vmem_limit_bytes=40 * 1024 * 1024
            ),
        )(g, m, w)

    specs = P("shift", "fsdp", "tp")
    return jax.shard_map(
        body, mesh=mesh, in_specs=(specs,) * 3, out_specs=(specs,) * 2, check_vma=False
    )
```

```python
import functools

import jax
import jax.numpy as jnp
from jax import lax
from jax.experimental import pallas as pl
from jax.experimental.pallas import tpu as pltpu
from jax.sharding import PartitionSpec as P

MESH = pl.DeviceIdType.MESH
ITERS = 3
hold_rate = 0.95
learn_rate = 0.9


def full_dot(a, b, dims):
    return lax.dot_general(
        a, b, (dims, ((), ())), precision=lax.Precision.HIGHEST, preferred_element_type=jnp.float32
    )


def times(a, b):
    return full_dot(a, b, ((1,), (0,)))


def polynomial(gram):
    side = gram.shape[0]
    eye = lax.broadcasted_iota(jnp.int32, (side, side), 0) == lax.broadcasted_iota(
        jnp.int32, (side, side), 1
    )
    total = jnp.sum(jnp.sum(jnp.where(eye, gram, 0.0), axis=1, keepdims=True), axis=0, keepdims=True)
    scale = lax.rsqrt(total + 1e-06)
    a = gram * (scale * scale)
    whole = None
    for step in range(ITERS):
        mixed = -4.775 * a + 2.0315 * times(a, a)
        mixed = jnp.where(eye, mixed + 3.4445, mixed)
        whole = mixed if whole is None else times(mixed, whole)
        if step < ITERS - 1:
            a = times(times(mixed, a), mixed)
    return whole * scale


def kernel(
    group,
    waves,
    g_ref,
    m_ref,
    w_ref,
    weights,
    momentum,
    g_buf,
    m_buf,
    w_buf,
    arrived,
    leaving,
    returned,
    rows,
    gram_out,
    gram_in,
    load_sem,
    w_sem,
    out_send,
    out_recv,
    gram_send,
    gram_recv,
    back_send,
    back_recv,
):
    me, half = lax.axis_index("fsdp"), lax.axis_index("tp")
    near, other = rows.shape[0] // group, lax.rem(half + 1, 2)

    def peer(o):
        return lax.rem(me + o, group)

    barrier = pltpu.get_barrier_semaphore()

    def greet(o, _):
        pl.semaphore_signal(barrier, inc=1, device_id={"fsdp": peer(o)}, device_id_type=MESH)
        return 0

    lax.fori_loop(1, group, greet, 0)
    pl.semaphore_signal(barrier, inc=1, device_id={"tp": other}, device_id_type=MESH)

    def part(w):
        return pl.ds(w * group, group)

    def loads(w):
        return (
            pltpu.make_async_copy(g_ref.at[part(w)], g_buf.at[part(w)], load_sem.at[0, w]),
            pltpu.make_async_copy(m_ref.at[part(w)], m_buf.at[part(w)], load_sem.at[1, w]),
        )

    for w in range(waves):
        for copy in loads(w):
            copy.start()
    w_copy = pltpu.make_async_copy(w_ref, w_buf, w_sem)
    w_copy.start()

    def out_copy(w, o):
        return pltpu.make_async_remote_copy(
            src_ref=momentum.at[w * group + peer(o)],
            dst_ref=arrived.at[w, me],
            send_sem=out_send.at[w],
            recv_sem=out_recv.at[w],
            device_id={"fsdp": peer(o)},
            device_id_type=MESH,
        )

    def back_copy(w, o):
        return pltpu.make_async_remote_copy(
            src_ref=leaving.at[w, peer(o)],
            dst_ref=returned.at[w * group + me],
            send_sem=back_send.at[w],
            recv_sem=back_recv.at[w],
            device_id={"fsdp": peer(o)},
            device_id_type=MESH,
        )

    def all_of(buf, send, recv):
        return pltpu.make_async_remote_copy(
            src_ref=buf, dst_ref=buf, send_sem=send, recv_sem=recv,
            device_id={"fsdp": me}, device_id_type=MESH,
        )

    def gram_copy(w):
        return pltpu.make_async_remote_copy(
            src_ref=gram_out.at[w],
            dst_ref=gram_in.at[w],
            send_sem=gram_send.at[w],
            recv_sem=gram_recv.at[w],
            device_id={"tp": other},
            device_id_type=MESH,
        )

    for w in range(waves):
        for copy in loads(w):
            copy.wait()
        momentum[part(w)] = hold_rate * m_buf[part(w)] + g_buf[part(w)]
        if w == 0:
            pl.semaphore_wait(barrier, group)

        def send(o, _, w=w):
            out_copy(w, o).start()
            return 0

        lax.fori_loop(1, group, send, 0)
        arrived[w, me] = momentum[w * group + me]

    def wave(w, _):
        all_of(arrived.at[w, pl.ds(0, group - 1)], out_send.at[w], out_recv.at[w]).wait_recv()
        for k in range(group // 2):
            rows[pl.ds(2 * near * k, 2 * near), :] = jnp.concatenate(
                [arrived[w, 2 * k], arrived[w, 2 * k + 1]], axis=0
            )
        mat = rows[...]
        gram_out[w] = full_dot(mat, mat, ((1,), (1,)))
        gram_copy(w).start()
        gram_copy(w).wait_recv()
        mix = polynomial(gram_out[w] + gram_in[w])
        product = times(mix, rows[...])
        for k in range(group):
            leaving[w, k] = product[near * k : near * (k + 1)]

        def send(o, _):
            back_copy(w, o).start()
            return 0

        lax.fori_loop(1, group, send, 0)
        returned[w * group + me] = leaving[w, me]
        return 0

    lax.fori_loop(0, waves, wave, 0)
    w_copy.wait()

    def finish(w, _):
        all_of(returned.at[pl.ds(w * group, group - 1)], back_send.at[w], back_recv.at[w]).wait_recv()
        weights[part(w)] = w_buf[part(w)] - learn_rate * returned[part(w)]
        return 0

    lax.fori_loop(0, waves, finish, 0)

    def drain(w, _):
        all_of(arrived.at[w, pl.ds(0, group - 1)], out_send.at[w], out_recv.at[w]).wait_send()
        gram_copy(w).wait_send()
        all_of(returned.at[pl.ds(w * group, group - 1)], back_send.at[w], back_recv.at[w]).wait_send()
        return 0

    lax.fori_loop(0, waves, drain, 0)


def solution(mesh):
    group = mesh.shape["fsdp"]

    def body(g, m, w):
        mats, near, wide = g.shape
        waves, side = mats // group, near * group
        block = jax.ShapeDtypeStruct(g.shape, jnp.float32)
        f32 = jnp.float32
        sem = pltpu.SemaphoreType.DMA
        return pl.pallas_call(
            functools.partial(kernel, group, waves),
            name="update",
            out_shape=(block, block),
            in_specs=[pl.BlockSpec(memory_space=pltpu.HBM)] * 3,
            out_specs=[pl.BlockSpec(memory_space=pltpu.VMEM)] * 2,
            scratch_shapes=[
                pltpu.VMEM(g.shape, f32),
                pltpu.VMEM(g.shape, f32),
                pltpu.VMEM(g.shape, f32),
                pltpu.VMEM((waves, group, near, wide), f32),
                pltpu.VMEM((waves, group, near, wide), f32),
                pltpu.VMEM(g.shape, f32),
                pltpu.VMEM((side, wide), f32),
                pltpu.VMEM((waves, side, side), f32),
                pltpu.VMEM((waves, side, side), f32),
                sem((2, waves)),
                sem,
                sem((waves,)),
                sem((waves,)),
                sem((waves,)),
                sem((waves,)),
                sem((waves,)),
                sem((waves,)),
            ],
            compiler_params=pltpu.CompilerParams(
                collective_id=0, has_side_effects=True, vmem_limit_bytes=48 * 1024 * 1024
            ),
        )(g, m, w)

    specs = P("shift", "fsdp", "tp")
    return jax.shard_map(
        body, mesh=mesh, in_specs=(specs,) * 3, out_specs=(specs,) * 2, check_vma=False
    )
```

```python
import functools

import jax
import jax.numpy as jnp
from jax import lax
from jax.experimental import pallas as pl
from jax.experimental.pallas import tpu as pltpu
from jax.sharding import PartitionSpec as P

MESH = pl.DeviceIdType.MESH
MIB = 1024 * 1024
ITERS = 3
hold_rate = 0.95
learn_rate = 0.9

def order():
    plus = [(dz, b, c) for b, c in ((0, 0), (1, 1), (0, 1), (1, 0)) for dz in (3, 2, 1)]
    minus = [(dz, b, c) for b, c in ((0, 0), (1, 1), (0, 1), (1, 0)) for dz in (5, 6, 7)]
    far = [(4, b, c) for b, c in ((0, 0), (1, 1), (0, 1), (1, 0))]
    out = []
    for i, pair in enumerate(zip(plus, minus)):
        out += pair
        if i % 3 == 2:
            out.append(far[i // 3])
    return out + [(0, 1, 0), (0, 0, 1), (0, 1, 1)]


def full_dot(a, b, dims):
    return lax.dot_general(
        a, b, (dims, ((), ())), precision=lax.Precision.HIGHEST, preferred_element_type=jnp.float32
    )


def times(a, b):
    return full_dot(a, b, ((1,), (0,)))


def polynomial(gram):
    side = gram.shape[0]
    eye = lax.broadcasted_iota(jnp.int32, (side, side), 0) == lax.broadcasted_iota(
        jnp.int32, (side, side), 1
    )
    total = jnp.sum(jnp.sum(jnp.where(eye, gram, 0.0), axis=1, keepdims=True), axis=0, keepdims=True)
    scale = lax.rsqrt(total + 1e-06)
    a = gram * (scale * scale)
    whole = None
    for step in range(ITERS):
        mixed = -4.775 * a + 2.0315 * times(a, a)
        mixed = jnp.where(eye, mixed + 3.4445, mixed)
        whole = mixed if whole is None else times(mixed, whole)
        if step < ITERS - 1:
            a = times(times(mixed, a), mixed)
    return whole * scale


def exchange(
    group,
    waves,
    g_ref,
    m_ref,
    w_ref,
    weights,
    momentum,
    last,
    g_buf,
    m_buf,
    arrived,
    leaving,
    returned,
    rows,
    gram_out,
    gram_in,
    load_sem,
    w_sem,
    out_send,
    out_recv,
    gram_send,
    gram_recv,
    back_send,
    back_recv,
):
    me, half = lax.axis_index("fsdp"), lax.axis_index("tp")
    near, other = rows.shape[0] // group, lax.rem(half + 1, 2)
    z, y, core = me // 4, lax.rem(me // 2, 2), lax.rem(me, 2)
    depth = group // 4

    def partner(step):
        dz, dy, dc = step
        return lax.rem(z + dz, depth) * 4 + lax.rem(y + dy, 2) * 2 + lax.rem(core + dc, 2)

    barrier = pltpu.get_barrier_semaphore()

    def greet(o, _):
        pl.semaphore_signal(
            barrier, inc=1, device_id={"fsdp": lax.rem(me + o, group)}, device_id_type=MESH
        )
        return 0

    lax.fori_loop(1, group, greet, 0)
    pl.semaphore_signal(barrier, inc=1, device_id={"tp": other}, device_id_type=MESH)

    def part(w):
        return pl.ds(w * group, group)

    def loads(w):
        return (
            pltpu.make_async_copy(g_ref.at[part(w)], g_buf.at[part(w)], load_sem.at[0, w]),
            pltpu.make_async_copy(m_ref.at[part(w)], m_buf.at[part(w)], load_sem.at[1, w]),
        )

    for w in range(waves):
        for copy in loads(w):
            copy.start()
    w_copy = pltpu.make_async_copy(w_ref, weights, w_sem)
    w_copy.start()

    def out_copy(w, to):
        return pltpu.make_async_remote_copy(
            src_ref=momentum.at[w * group + to],
            dst_ref=arrived.at[w, me],
            send_sem=out_send.at[w],
            recv_sem=out_recv.at[w],
            device_id={"fsdp": to},
            device_id_type=MESH,
        )

    def back_copy(w, to):
        return pltpu.make_async_remote_copy(
            src_ref=leaving.at[w, to],
            dst_ref=returned.at[w, me],
            send_sem=back_send.at[w],
            recv_sem=back_recv.at[w],
            device_id={"fsdp": to},
            device_id_type=MESH,
        )

    def all_of(buf, w, send, recv):
        blocks = buf.at[w, pl.ds(0, group - 1)]
        return pltpu.make_async_remote_copy(
            src_ref=blocks, dst_ref=blocks, send_sem=send.at[w], recv_sem=recv.at[w],
            device_id={"fsdp": me}, device_id_type=MESH,
        )

    def gram_copy(w):
        return pltpu.make_async_remote_copy(
            src_ref=gram_out.at[w],
            dst_ref=gram_in.at[w],
            send_sem=gram_send.at[w],
            recv_sem=gram_recv.at[w],
            device_id={"tp": other},
            device_id_type=MESH,
        )

    for w in range(waves):
        for copy in loads(w):
            copy.wait()
        momentum[part(w)] = hold_rate * m_buf[part(w)] + g_buf[part(w)]
        arrived[w, me] = momentum[w * group + me]
    pl.semaphore_wait(barrier, group)

    def send_out(w, _):
        for step in order():
            out_copy(w, partner(step)).start()
        return 0

    lax.fori_loop(0, waves, send_out, 0)

    def wave(w, _):
        all_of(arrived, w, out_send, out_recv).wait_recv()
        for k in range(group // 2):
            rows[pl.ds(2 * near * k, 2 * near), :] = jnp.concatenate(
                [arrived[w, 2 * k], arrived[w, 2 * k + 1]], axis=0
            )
        mat = rows[...]
        gram_out[w] = full_dot(mat, mat, ((1,), (1,)))
        gram_copy(w).start()
        gram_copy(w).wait_recv()
        mix = polynomial(gram_out[w] + gram_in[w])
        product = times(mix, rows[...])
        for k in range(group):
            leaving[w, k] = product[near * k : near * (k + 1)]
        for step in order():
            back_copy(w, partner(step)).start()
        returned[w, me] = leaving[w, me]
        return 0

    lax.fori_loop(0, waves, wave, 0)
    w_copy.wait()

    def finish(w, _):
        all_of(returned, w, back_send, back_recv).wait_recv()
        weights[part(w)] = weights[part(w)] - learn_rate * returned[w]
        return 0

    lax.fori_loop(0, waves - 1, finish, 0)

    def drain(w, _):
        all_of(arrived, w, out_send, out_recv).wait_send()
        gram_copy(w).wait_send()
        all_of(returned, w, back_send, back_recv).wait_send()
        return 0

    lax.fori_loop(0, waves, drain, 0)
    all_of(returned, waves - 1, back_send, back_recv).wait_recv()
    last[...] = returned[waves - 1]


def store(weights, momentum, last, weights_out, momentum_out, fresh, sem):
    done = weights.shape[0] - last.shape[0]
    tail = pl.ds(done, last.shape[0])
    copies = [
        pltpu.make_async_copy(weights.at[pl.ds(0, done)], weights_out.at[pl.ds(0, done)], sem.at[0]),
        pltpu.make_async_copy(momentum, momentum_out, sem.at[1]),
        pltpu.make_async_copy(fresh, weights_out.at[tail], sem.at[2]),
    ]
    copies[0].start()
    copies[1].start()
    fresh[...] = weights[tail] - learn_rate * last[...]
    copies[2].start()
    for copy in copies:
        copy.wait()


def solution(mesh):
    group = mesh.shape["fsdp"]

    def body(g, m, w):
        mats, near, wide = g.shape
        waves, side = mats // group, near * group
        f32 = jnp.float32
        block = jax.ShapeDtypeStruct(g.shape, f32)
        fifth = jax.ShapeDtypeStruct((group, near, wide), f32)
        sem = pltpu.SemaphoreType.DMA
        in_hbm, in_vmem = pl.BlockSpec(memory_space=pltpu.HBM), pl.BlockSpec(memory_space=pltpu.VMEM)
        blocks = pltpu.VMEM((waves, group, near, wide), f32)
        squares = pltpu.VMEM((waves, side, side), f32)
        weights, momentum, last = pl.pallas_call(
            functools.partial(exchange, group, waves),
            name="update",
            out_shape=(block, block, fifth),
            in_specs=[in_hbm] * 3,
            out_specs=[in_vmem] * 3,
            scratch_shapes=[
                pltpu.VMEM(g.shape, f32),
                pltpu.VMEM(g.shape, f32),
                blocks,
                blocks,
                blocks,
                pltpu.VMEM((side, wide), f32),
                squares,
                squares,
                sem((2, waves)),
                sem,
                sem((waves,)),
                sem((waves,)),
                sem((waves,)),
                sem((waves,)),
                sem((waves,)),
                sem((waves,)),
            ],
            compiler_params=pltpu.CompilerParams(
                collective_id=0, has_side_effects=True, vmem_limit_bytes=48 * MIB
            ),
        )(g, m, w)
        return pl.pallas_call(
            store,
            name="store",
            out_shape=(block, block),
            in_specs=[in_vmem] * 3,
            out_specs=[in_hbm] * 2,
            scratch_shapes=[pltpu.VMEM(fifth.shape, f32), sem((3,))],
            compiler_params=pltpu.CompilerParams(vmem_limit_bytes=16 * MIB),
        )(weights, momentum, last)

    specs = P("shift", "fsdp", "tp")
    return jax.shard_map(
        body, mesh=mesh, in_specs=(specs,) * 3, out_specs=(specs,) * 2, check_vma=False
    )
```

```python
import functools

import jax
import jax.numpy as jnp
from jax import lax
from jax.experimental import pallas as pl
from jax.experimental.pallas import tpu as pltpu
from jax.sharding import PartitionSpec as P

MESH = pl.DeviceIdType.MESH
MIB = 1024 * 1024
ITERS = 3
hold_rate = 0.95
learn_rate = 0.9

def order():
    plus = [(dz, b, c) for b, c in ((0, 0), (1, 1), (0, 1), (1, 0)) for dz in (3, 2, 1)]
    minus = [(dz, b, c) for b, c in ((0, 0), (1, 1), (0, 1), (1, 0)) for dz in (5, 6, 7)]
    far = [(4, b, c) for b, c in ((0, 0), (1, 1), (0, 1), (1, 0))]
    out = []
    for i, pair in enumerate(zip(plus, minus)):
        out += pair
        if i % 3 == 2:
            out.append(far[i // 3])
    return out + [(0, 1, 0), (0, 0, 1), (0, 1, 1)]


def full_dot(a, b, dims):
    return lax.dot_general(
        a, b, (dims, ((), ())), precision=lax.Precision.HIGHEST, preferred_element_type=jnp.float32
    )


def times(a, b):
    return full_dot(a, b, ((1,), (0,)))


def polynomial(gram):
    side = gram.shape[0]
    eye = lax.broadcasted_iota(jnp.int32, (side, side), 0) == lax.broadcasted_iota(
        jnp.int32, (side, side), 1
    )
    total = jnp.sum(jnp.sum(jnp.where(eye, gram, 0.0), axis=1, keepdims=True), axis=0, keepdims=True)
    scale = lax.rsqrt(total + 1e-06)
    a = gram * (scale * scale)
    whole = None
    for step in range(ITERS):
        mixed = -4.775 * a + 2.0315 * times(a, a)
        mixed = jnp.where(eye, mixed + 3.4445, mixed)
        whole = mixed if whole is None else times(mixed, whole)
        if step < ITERS - 1:
            a = times(times(mixed, a), mixed)
    return whole * scale


def exchange(
    group,
    waves,
    g_ref,
    m_ref,
    w_ref,
    weights,
    momentum,
    returned,
    g_buf,
    m_buf,
    arrived,
    leaving,
    rows,
    gram_out,
    gram_in,
    load_sem,
    w_sem,
    out_send,
    out_recv,
    gram_send,
    gram_recv,
    back_send,
    back_recv,
    up_sem,
    down_sem,
):
    me, half = lax.axis_index("fsdp"), lax.axis_index("tp")
    near, other = rows.shape[0] // group, lax.rem(half + 1, 2)
    z, y, core = me // 4, lax.rem(me // 2, 2), lax.rem(me, 2)
    depth = group // 4

    def partner(step):
        dz, dy, dc = step
        return lax.rem(z + dz, depth) * 4 + lax.rem(y + dy, 2) * 2 + lax.rem(core + dc, 2)

    barrier = pltpu.get_barrier_semaphore()

    close = [step for step in order() if step[0] in (0, 1, depth - 1)]
    for step in close:
        pl.semaphore_signal(barrier, inc=1, device_id={"fsdp": partner(step)}, device_id_type=MESH)
    pl.semaphore_signal(barrier, inc=1, device_id={"tp": other}, device_id_type=MESH)

    def tell(sem, dz):
        pl.semaphore_signal(
            sem, inc=1, device_id={"fsdp": partner((dz, 0, 0))}, device_id_type=MESH
        )

    def part(w):
        return pl.ds(w * group, group)

    def loads(w):
        return (
            pltpu.make_async_copy(g_ref.at[part(w)], g_buf.at[part(w)], load_sem.at[0, w]),
            pltpu.make_async_copy(m_ref.at[part(w)], m_buf.at[part(w)], load_sem.at[1, w]),
        )

    for w in range(waves):
        for copy in loads(w):
            copy.start()
    w_copy = pltpu.make_async_copy(w_ref, weights, w_sem)
    w_copy.start()

    def out_copy(w, to):
        return pltpu.make_async_remote_copy(
            src_ref=momentum.at[w * group + to],
            dst_ref=arrived.at[w, me],
            send_sem=out_send.at[w],
            recv_sem=out_recv.at[w],
            device_id={"fsdp": to},
            device_id_type=MESH,
        )

    def back_copy(w, to):
        return pltpu.make_async_remote_copy(
            src_ref=leaving.at[w, to],
            dst_ref=returned.at[w, me],
            send_sem=back_send.at[w],
            recv_sem=back_recv.at[w],
            device_id={"fsdp": to},
            device_id_type=MESH,
        )

    def all_of(buf, w, send, recv):
        blocks = buf.at[w, pl.ds(0, group - 1)]
        return pltpu.make_async_remote_copy(
            src_ref=blocks, dst_ref=blocks, send_sem=send.at[w], recv_sem=recv.at[w],
            device_id={"fsdp": me}, device_id_type=MESH,
        )

    def gram_copy(w):
        return pltpu.make_async_remote_copy(
            src_ref=gram_out.at[w],
            dst_ref=gram_in.at[w],
            send_sem=gram_send.at[w],
            recv_sem=gram_recv.at[w],
            device_id={"tp": other},
            device_id_type=MESH,
        )

    def momenta(w):
        for copy in loads(w):
            copy.wait()
        momentum[part(w)] = hold_rate * m_buf[part(w)] + g_buf[part(w)]
        arrived[w, me] = momentum[w * group + me]

    def first_out(*distances):
        for step in order():
            if step[0] in distances:
                out_copy(0, partner(step)).start()

    momenta(0)
    pl.semaphore_wait(barrier, len(close) + 1)
    tell(up_sem.at[0], 1)
    tell(down_sem.at[0], depth - 1)
    first_out(0, 1, depth - 1)
    for hop in range(1, depth // 2):
        momenta(hop)
        pl.semaphore_wait(up_sem.at[hop - 1], 1)
        if hop < depth // 2 - 1:
            tell(up_sem.at[hop], 1)
            pl.semaphore_wait(down_sem.at[hop - 1], 1)
            if hop < depth // 2 - 2:
                tell(down_sem.at[hop], depth - 1)
            first_out(hop + 1, depth - hop - 1)
        else:
            first_out(hop + 1)

    def send_out(w, _):
        for step in order():
            out_copy(w, partner(step)).start()
        return 0

    lax.fori_loop(1, waves, send_out, 0)

    def wave(w, _):
        all_of(arrived, w, out_send, out_recv).wait_recv()
        for k in range(group // 2):
            rows[pl.ds(2 * near * k, 2 * near), :] = jnp.concatenate(
                [arrived[w, 2 * k], arrived[w, 2 * k + 1]], axis=0
            )
        mat = rows[...]
        gram_out[w] = full_dot(mat, mat, ((1,), (1,)))
        gram_copy(w).start()
        gram_copy(w).wait_recv()
        mix = polynomial(gram_out[w] + gram_in[w])
        product = times(mix, rows[...])
        for k in range(group):
            leaving[w, k] = product[near * k : near * (k + 1)]
        @pl.when(w < waves - 2)
        def _():
            for step in order():
                back_copy(w, partner(step)).start()

        @pl.when(w >= waves - 2)
        def _():
            for to_z in (0, 1, 2, 3, 7, 4, 6, 5):
                for b, c in ((1, 1), (0, 1), (1, 0), (0, 0)):
                    to = to_z * 4 + lax.rem(y + b, 2) * 2 + lax.rem(core + c, 2)
                    if b or c:
                        back_copy(w, to).start()
                    else:
                        @pl.when(to != me)
                        def _(to=to):
                            back_copy(w, to).start()

        returned[w, me] = leaving[w, me]
        return 0

    lax.fori_loop(0, waves, wave, 0)
    w_copy.wait()

    def finish(w, _):
        all_of(returned, w, back_send, back_recv).wait_recv()
        weights[part(w)] = weights[part(w)] - learn_rate * returned[w]
        return 0

    lax.fori_loop(0, waves - 1, finish, 0)

    def drain(w, _):
        all_of(arrived, w, out_send, out_recv).wait_send()
        gram_copy(w).wait_send()
        all_of(returned, w, back_send, back_recv).wait_send()
        return 0

    lax.fori_loop(0, waves, drain, 0)
    all_of(returned, waves - 1, back_send, back_recv).wait_recv()


def store(weights, momentum, returned, weights_out, momentum_out, fresh, sem):
    waves, group = returned.shape[:2]
    done, tail = pl.ds(0, (waves - 1) * group), pl.ds((waves - 1) * group, group)
    copies = [
        pltpu.make_async_copy(weights.at[done], weights_out.at[done], sem.at[0]),
        pltpu.make_async_copy(momentum, momentum_out, sem.at[1]),
        pltpu.make_async_copy(fresh, weights_out.at[tail], sem.at[2]),
    ]
    copies[0].start()
    copies[1].start()
    fresh[...] = weights[tail] - learn_rate * returned[waves - 1]
    copies[2].start()
    for copy in copies:
        copy.wait()


def solution(mesh):
    group = mesh.shape["fsdp"]

    def body(g, m, w):
        mats, near, wide = g.shape
        waves, side = mats // group, near * group
        f32 = jnp.float32
        block = jax.ShapeDtypeStruct(g.shape, f32)
        sem = pltpu.SemaphoreType.DMA
        in_hbm, in_vmem = pl.BlockSpec(memory_space=pltpu.HBM), pl.BlockSpec(memory_space=pltpu.VMEM)
        blocks = pltpu.VMEM((waves, group, near, wide), f32)
        split = jax.ShapeDtypeStruct(blocks.shape, f32)
        squares = pltpu.VMEM((waves, side, side), f32)
        weights, momentum, returned = pl.pallas_call(
            functools.partial(exchange, group, waves),
            name="update",
            out_shape=(block, block, split),
            in_specs=[in_hbm] * 3,
            out_specs=[in_vmem] * 3,
            scratch_shapes=[
                pltpu.VMEM(g.shape, f32),
                pltpu.VMEM(g.shape, f32),
                blocks,
                blocks,
                pltpu.VMEM((side, wide), f32),
                squares,
                squares,
                sem((2, waves)),
                sem,
                sem((waves,)),
                sem((waves,)),
                sem((waves,)),
                sem((waves,)),
                sem((waves,)),
                sem((waves,)),
                pltpu.SemaphoreType.REGULAR((group // 8 - 1,)),
                pltpu.SemaphoreType.REGULAR((group // 8 - 2,)),
            ],
            compiler_params=pltpu.CompilerParams(
                collective_id=0, has_side_effects=True, vmem_limit_bytes=46 * MIB
            ),
        )(g, m, w)
        return pl.pallas_call(
            store,
            name="store",
            out_shape=(block, block),
            in_specs=[in_vmem] * 3,
            out_specs=[in_hbm] * 2,
            scratch_shapes=[pltpu.VMEM((group, near, wide), f32), sem((3,))],
            compiler_params=pltpu.CompilerParams(vmem_limit_bytes=16 * MIB),
        )(weights, momentum, returned)

    specs = P("shift", "fsdp", "tp")
    return jax.shard_map(
        body, mesh=mesh, in_specs=(specs,) * 3, out_specs=(specs,) * 2, check_vma=False
    )
```

```python
import functools

import jax
import jax.numpy as jnp
from jax import lax
from jax.experimental import pallas as pl
from jax.experimental.pallas import tpu as pltpu
from jax.sharding import PartitionSpec as P

MESH = pl.DeviceIdType.MESH
MIB = 1024 * 1024
ITERS = 3
hold_rate = 0.95
learn_rate = 0.9

CORNERS = ((1, 1), (0, 1), (1, 0), (0, 0))


def order():
    steps = [(dz, b, c) for dz in (5, 4, 3, 6, 2, 7, 1, 0) for b, c in CORNERS]
    return [step for step in steps if any(step)]


def full_dot(a, b, dims):
    return lax.dot_general(
        a, b, (dims, ((), ())), precision=lax.Precision.HIGHEST, preferred_element_type=jnp.float32
    )


def times(a, b):
    return full_dot(a, b, ((1,), (0,)))


def polynomial(gram):
    side = gram.shape[0]
    eye = lax.broadcasted_iota(jnp.int32, (side, side), 0) == lax.broadcasted_iota(
        jnp.int32, (side, side), 1
    )
    total = jnp.sum(jnp.sum(jnp.where(eye, gram, 0.0), axis=1, keepdims=True), axis=0, keepdims=True)
    scale = lax.rsqrt(total + 1e-06)
    a = gram * (scale * scale)
    whole = None
    for step in range(ITERS):
        mixed = -4.775 * a + 2.0315 * times(a, a)
        mixed = jnp.where(eye, mixed + 3.4445, mixed)
        whole = mixed if whole is None else times(mixed, whole)
        if step < ITERS - 1:
            a = times(times(mixed, a), mixed)
    return whole * scale


def exchange(
    group,
    waves,
    g_ref,
    m_ref,
    w_ref,
    weights,
    momentum,
    returned,
    g_buf,
    m_buf,
    arrived,
    leaving,
    rows,
    gram_out,
    gram_in,
    load_sem,
    w_sem,
    out_send,
    out_recv,
    gram_send,
    gram_recv,
    back_send,
    back_recv,
    up_sem,
    down_sem,
    side_sem,
):
    me, half = lax.axis_index("fsdp"), lax.axis_index("tp")
    near, other = rows.shape[0] // group, lax.rem(half + 1, 2)
    z, y, core = me // 4, lax.rem(me // 2, 2), lax.rem(me, 2)
    depth = group // 4

    def partner(step):
        dz, dy, dc = step
        turned = lax.rem(z, 2) * (depth - 2 * dz)
        return lax.rem(z + dz + turned, depth) * 4 + lax.rem(y + dy, 2) * 2 + lax.rem(core + dc, 2)

    def part(w):
        return pl.ds(w * group, group)

    barrier = pltpu.get_barrier_semaphore()

    def loads(w):
        return (
            pltpu.make_async_copy(g_ref.at[part(w)], g_buf.at[part(w)], load_sem.at[0, w]),
            pltpu.make_async_copy(m_ref.at[part(w)], m_buf.at[part(w)], load_sem.at[1, w]),
        )

    for copy in loads(0):
        copy.start()
    close = [s for s in order() if s[0] == 0 or s[0] in (1, depth - 1) and s[1] == 0]
    close.sort(key=lambda s: s[0] == 0)
    beside = {"fsdp": partner((0, 1, 0)), "tp": other}
    for step in close:
        pl.semaphore_signal(barrier, inc=1, device_id={"fsdp": partner(step)}, device_id_type=MESH)
    pl.semaphore_signal(barrier, inc=1, device_id=beside, device_id_type=MESH)
    for w in range(1, waves):
        for copy in loads(w):
            copy.start()

    def tell(sem, dz):
        to = lax.rem(me + 4 * dz, group)
        pl.semaphore_signal(sem, inc=1, device_id={"fsdp": to}, device_id_type=MESH)

    w_copy = pltpu.make_async_copy(w_ref, weights, w_sem)
    w_copy.start()

    def out_copy(w, to):
        return pltpu.make_async_remote_copy(
            src_ref=momentum.at[w * group + to],
            dst_ref=arrived.at[w, me],
            send_sem=out_send.at[w],
            recv_sem=out_recv.at[w],
            device_id={"fsdp": to},
            device_id_type=MESH,
        )

    def back_copy(w, to):
        return pltpu.make_async_remote_copy(
            src_ref=leaving.at[w, to],
            dst_ref=returned.at[w, me],
            send_sem=back_send.at[w],
            recv_sem=back_recv.at[w],
            device_id={"fsdp": to},
            device_id_type=MESH,
        )

    def all_of(buf, w, send, recv):
        blocks = buf.at[w, pl.ds(0, group - 1)]
        return pltpu.make_async_remote_copy(
            src_ref=blocks, dst_ref=blocks, send_sem=send.at[w], recv_sem=recv.at[w],
            device_id={"fsdp": me}, device_id_type=MESH,
        )

    def gram_copy(w):
        return pltpu.make_async_remote_copy(
            src_ref=gram_out.at[w],
            dst_ref=gram_in.at[w],
            send_sem=gram_send.at[w],
            recv_sem=gram_recv.at[w],
            device_id={"tp": other},
            device_id_type=MESH,
        )

    def momenta(w):
        for copy in loads(w):
            copy.wait()
        momentum[part(w)] = hold_rate * m_buf[part(w)] + g_buf[part(w)]
        arrived[w, me] = momentum[w * group + me]

    def first_out(hop):
        for dz, b, c in sorted(order(), key=lambda s: s[0] == 0):
            hops = min(dz, depth - dz)
            if hops == hop + 1 - b or hops == hop == 0:
                out_copy(0, partner((dz, b, c))).start()

    far = depth // 2
    momenta(0)
    pl.semaphore_wait(barrier, len(close) + 1)
    tell(up_sem.at[0], 1)
    tell(down_sem.at[0], depth - 1)
    first_out(0)
    pl.semaphore_signal(side_sem, inc=1, device_id=beside, device_id_type=MESH)
    for hop in range(1, far + 1):
        if hop < waves:
            momenta(hop)
        pl.semaphore_wait(up_sem.at[hop - 1], 1)
        if hop < far:
            tell(up_sem.at[hop], 1)
            pl.semaphore_wait(down_sem.at[hop - 1], 1)
            if hop < far - 1:
                tell(down_sem.at[hop], depth - 1)
        first_out(hop)
    pl.semaphore_wait(side_sem, 1)

    def send_out(w, _):
        for step in order():
            out_copy(w, partner(step)).start()
        return 0

    lax.fori_loop(1, waves, send_out, 0)

    def wave(w, _):
        all_of(arrived, w, out_send, out_recv).wait_recv()
        for k in range(group // 2):
            rows[pl.ds(2 * near * k, 2 * near), :] = jnp.concatenate(
                [arrived[w, 2 * k], arrived[w, 2 * k + 1]], axis=0
            )
        mat = rows[...]
        gram_out[w] = full_dot(mat, mat, ((1,), (1,)))
        gram_copy(w).start()
        gram_copy(w).wait_recv()
        mix = polynomial(gram_out[w] + gram_in[w])
        product = times(mix, rows[...])
        for k in range(group):
            leaving[w, k] = product[near * k : near * (k + 1)]
        @pl.when(w < waves - 2)
        def _():
            for step in order():
                back_copy(w, partner(step)).start()

        @pl.when(w >= waves - 2)
        def _():
            for to_z in (0,):
                for b, c in CORNERS:
                    to = to_z * 4 + lax.rem(y + b, 2) * 2 + lax.rem(core + c, 2)

                    @pl.when(to != me)
                    def _(to=to):
                        back_copy(w, to).start()

            for step in order():
                to = partner(step)

                @pl.when(to >= 4)
                def _(to=to):
                    back_copy(w, to).start()

        returned[w, me] = leaving[w, me]
        return 0

    lax.fori_loop(0, waves, wave, 0)
    w_copy.wait()

    def finish(w, _):
        all_of(returned, w, back_send, back_recv).wait_recv()
        weights[part(w)] = weights[part(w)] - learn_rate * returned[w]
        return 0

    lax.fori_loop(0, waves - 1, finish, 0)

    def drain(w, _):
        all_of(arrived, w, out_send, out_recv).wait_send()
        gram_copy(w).wait_send()
        all_of(returned, w, back_send, back_recv).wait_send()
        return 0

    lax.fori_loop(0, waves, drain, 0)
    all_of(returned, waves - 1, back_send, back_recv).wait_recv()


def store(weights, momentum, returned, weights_out, momentum_out, fresh, sem):
    waves, group = returned.shape[:2]
    done, tail = pl.ds(0, (waves - 1) * group), pl.ds((waves - 1) * group, group)
    copies = [
        pltpu.make_async_copy(weights.at[done], weights_out.at[done], sem.at[0]),
        pltpu.make_async_copy(momentum, momentum_out, sem.at[1]),
        pltpu.make_async_copy(fresh, weights_out.at[tail], sem.at[2]),
    ]
    copies[0].start()
    copies[1].start()
    fresh[...] = weights[tail] - learn_rate * returned[waves - 1]
    copies[2].start()
    for copy in copies:
        copy.wait()


def solution(mesh):
    group = mesh.shape["fsdp"]

    def body(g, m, w):
        mats, near, wide = g.shape
        waves, side = mats // group, near * group
        f32 = jnp.float32
        block = jax.ShapeDtypeStruct(g.shape, f32)
        sem = pltpu.SemaphoreType.DMA
        in_hbm, in_vmem = pl.BlockSpec(memory_space=pltpu.HBM), pl.BlockSpec(memory_space=pltpu.VMEM)
        blocks = pltpu.VMEM((waves, group, near, wide), f32)
        split = jax.ShapeDtypeStruct(blocks.shape, f32)
        squares = pltpu.VMEM((waves, side, side), f32)
        weights, momentum, returned = pl.pallas_call(
            functools.partial(exchange, group, waves),
            name="update",
            out_shape=(block, block, split),
            in_specs=[in_hbm] * 3,
            out_specs=[in_vmem] * 3,
            scratch_shapes=[
                pltpu.VMEM(g.shape, f32),
                pltpu.VMEM(g.shape, f32),
                blocks,
                blocks,
                pltpu.VMEM((side, wide), f32),
                squares,
                squares,
                sem((2, waves)),
                sem,
                sem((waves,)),
                sem((waves,)),
                sem((waves,)),
                sem((waves,)),
                sem((waves,)),
                sem((waves,)),
                pltpu.SemaphoreType.REGULAR((group // 8,)),
                pltpu.SemaphoreType.REGULAR((group // 8 - 1,)),
                pltpu.SemaphoreType.REGULAR,
            ],
            compiler_params=pltpu.CompilerParams(
                collective_id=0, has_side_effects=True, vmem_limit_bytes=46 * MIB
            ),
        )(g, m, w)
        return pl.pallas_call(
            store,
            name="store",
            out_shape=(block, block),
            in_specs=[in_vmem] * 3,
            out_specs=[in_hbm] * 2,
            scratch_shapes=[pltpu.VMEM((group, near, wide), f32), sem((3,))],
            compiler_params=pltpu.CompilerParams(vmem_limit_bytes=16 * MIB),
        )(weights, momentum, returned)

    specs = P("shift", "fsdp", "tp")
    return jax.shard_map(
        body, mesh=mesh, in_specs=(specs,) * 3, out_specs=(specs,) * 2, check_vma=False
    )
```

```python
import functools

import jax
import jax.numpy as jnp
from jax import lax
from jax.experimental import pallas as pl
from jax.experimental.pallas import tpu as pltpu
from jax.sharding import PartitionSpec as P

MESH = pl.DeviceIdType.MESH
MIB = 1024 * 1024
ITERS = 3
hold_rate = 0.95
learn_rate = 0.9

CORNERS = ((1, 1), (0, 1), (1, 0), (0, 0))


def order():
    steps = [(dz, b, c) for dz in (5, 4, 3, 6, 2, 7, 1, 0) for b, c in CORNERS]
    return [step for step in steps if any(step)]


def full_dot(a, b, dims):
    return lax.dot_general(
        a, b, (dims, ((), ())), precision=lax.Precision.HIGHEST, preferred_element_type=jnp.float32
    )


def times(a, b):
    return full_dot(a, b, ((1,), (0,)))


def polynomial(gram):
    side = gram.shape[0]
    eye = lax.broadcasted_iota(jnp.int32, (side, side), 0) == lax.broadcasted_iota(
        jnp.int32, (side, side), 1
    )
    total = jnp.sum(jnp.sum(jnp.where(eye, gram, 0.0), axis=1, keepdims=True), axis=0, keepdims=True)
    scale = lax.rsqrt(total + 1e-06)
    a = gram * (scale * scale)
    whole = None
    for step in range(ITERS):
        mixed = -4.775 * a + 2.0315 * times(a, a)
        mixed = jnp.where(eye, mixed + 3.4445, mixed)
        whole = mixed if whole is None else times(mixed, whole)
        if step < ITERS - 1:
            a = times(times(mixed, a), mixed)
    return whole * scale


def exchange(
    group,
    waves,
    g_ref,
    m_ref,
    w_ref,
    weights,
    momentum,
    returned,
    g_buf,
    m_buf,
    arrived,
    leaving,
    rows,
    gram_out,
    gram_in,
    load_sem,
    w_sem,
    out_send,
    out_recv,
    gram_send,
    gram_recv,
    back_send,
    back_recv,
    up_sem,
    down_sem,
    side_sem,
):
    me, half = lax.axis_index("fsdp"), lax.axis_index("tp")
    near, other = rows.shape[0] // group, lax.rem(half + 1, 2)
    z, y, core = me // 4, lax.rem(me // 2, 2), lax.rem(me, 2)
    depth = group // 4

    def partner(step):
        dz, dy, dc = step
        turned = lax.rem(z, 2) * (depth - 2 * dz)
        return lax.rem(z + dz + turned, depth) * 4 + lax.rem(y + dy, 2) * 2 + lax.rem(core + dc, 2)

    def part(w):
        return pl.ds(w * group, group)

    barrier = pltpu.get_barrier_semaphore()

    def loads(w):
        return (
            pltpu.make_async_copy(g_ref.at[part(w)], g_buf.at[part(w)], load_sem.at[0, w]),
            pltpu.make_async_copy(m_ref.at[part(w)], m_buf.at[part(w)], load_sem.at[1, w]),
        )

    for copy in loads(0):
        copy.start()
    close = [s for s in order() if s[0] == 0 or s[0] in (1, depth - 1) and s[1] == 0]
    close.sort(key=lambda s: s[0] == 0)
    beside = {"fsdp": partner((0, 1, 0)), "tp": other}
    for step in close:
        pl.semaphore_signal(barrier, inc=1, device_id={"fsdp": partner(step)}, device_id_type=MESH)
    pl.semaphore_signal(barrier, inc=1, device_id=beside, device_id_type=MESH)
    for w in range(1, waves):
        for copy in loads(w):
            copy.start()

    def tell(sem, dz):
        to = lax.rem(me + 4 * dz, group)
        pl.semaphore_signal(sem, inc=1, device_id={"fsdp": to}, device_id_type=MESH)

    w_copy = pltpu.make_async_copy(w_ref, weights, w_sem)
    w_copy.start()

    def out_copy(w, to):
        return pltpu.make_async_remote_copy(
            src_ref=momentum.at[w * group + to],
            dst_ref=arrived.at[w, me],
            send_sem=out_send.at[w],
            recv_sem=out_recv.at[w],
            device_id={"fsdp": to},
            device_id_type=MESH,
        )

    def back_copy(w, to):
        return pltpu.make_async_remote_copy(
            src_ref=leaving.at[w, to],
            dst_ref=returned.at[w, me],
            send_sem=back_send.at[w],
            recv_sem=back_recv.at[w],
            device_id={"fsdp": to},
            device_id_type=MESH,
        )

    def all_of(buf, w, send, recv):
        blocks = buf.at[w, pl.ds(0, group - 1)]
        return pltpu.make_async_remote_copy(
            src_ref=blocks, dst_ref=blocks, send_sem=send.at[w], recv_sem=recv.at[w],
            device_id={"fsdp": me}, device_id_type=MESH,
        )

    def gram_copy(w):
        return pltpu.make_async_remote_copy(
            src_ref=gram_out.at[w],
            dst_ref=gram_in.at[w],
            send_sem=gram_send.at[w],
            recv_sem=gram_recv.at[w],
            device_id={"tp": other},
            device_id_type=MESH,
        )

    def momenta(w):
        for copy in loads(w):
            copy.wait()
        momentum[part(w)] = hold_rate * m_buf[part(w)] + g_buf[part(w)]
        arrived[w, me] = momentum[w * group + me]

    def first_out(hop):
        for dz, b, c in sorted(order(), key=lambda s: s[0] == 0):
            hops = min(dz, depth - dz)
            if hops == hop + 1 - b or hops == hop == 0:
                out_copy(0, partner((dz, b, c))).start()

    far = depth // 2
    momenta(0)
    pl.semaphore_wait(barrier, len(close) + 1)
    tell(up_sem.at[0], 1)
    tell(down_sem.at[0], depth - 1)
    first_out(0)
    pl.semaphore_signal(side_sem, inc=1, device_id=beside, device_id_type=MESH)
    for hop in range(1, far + 1):
        if hop < waves:
            momenta(hop)
        pl.semaphore_wait(up_sem.at[hop - 1], 1)
        if hop < far:
            tell(up_sem.at[hop], 1)
            pl.semaphore_wait(down_sem.at[hop - 1], 1)
            if hop < far - 1:
                tell(down_sem.at[hop], depth - 1)
        first_out(hop)
    pl.semaphore_wait(side_sem, 1)

    def send_out(w, _):
        for step in order():
            out_copy(w, partner(step)).start()
        return 0

    lax.fori_loop(1, waves, send_out, 0)

    def wave(w, _):
        all_of(arrived, w, out_send, out_recv).wait_recv()
        for k in range(group // 2):
            rows[pl.ds(2 * near * k, 2 * near), :] = jnp.concatenate(
                [arrived[w, 2 * k], arrived[w, 2 * k + 1]], axis=0
            )
        mat = rows[...]
        gram_out[w] = full_dot(mat, mat, ((1,), (1,)))
        gram_copy(w).start()
        gram_copy(w).wait_recv()
        mix = polynomial(gram_out[w] + gram_in[w])
        product = times(mix, rows[...])
        for k in range(group):
            leaving[w, k] = product[near * k : near * (k + 1)]
        @pl.when(w < waves - 1)
        def _():
            for step in order():
                back_copy(w, partner(step)).start()

        @pl.when(w >= waves - 1)
        def _():
            for to_z in (0, 1, 2, 3, 7, 4, 6, 5):
                for b, c in CORNERS:
                    to = to_z * 4 + lax.rem(y + b, 2) * 2 + lax.rem(core + c, 2)
                    if b or c:
                        back_copy(w, to).start()
                    else:
                        @pl.when(to != me)
                        def _(to=to):
                            back_copy(w, to).start()

        returned[w, me] = leaving[w, me]
        return 0

    lax.fori_loop(0, waves, wave, 0)
    w_copy.wait()

    def finish(w, _):
        all_of(returned, w, back_send, back_recv).wait_recv()
        weights[part(w)] = weights[part(w)] - learn_rate * returned[w]
        return 0

    lax.fori_loop(0, waves - 1, finish, 0)

    def drain(w, _):
        all_of(arrived, w, out_send, out_recv).wait_send()
        gram_copy(w).wait_send()
        all_of(returned, w, back_send, back_recv).wait_send()
        return 0

    lax.fori_loop(0, waves, drain, 0)
    all_of(returned, waves - 1, back_send, back_recv).wait_recv()


def store(weights, momentum, returned, weights_out, momentum_out, fresh, sem):
    waves, group = returned.shape[:2]
    done, tail = pl.ds(0, (waves - 1) * group), pl.ds((waves - 1) * group, group)
    copies = [
        pltpu.make_async_copy(weights.at[done], weights_out.at[done], sem.at[0]),
        pltpu.make_async_copy(momentum, momentum_out, sem.at[1]),
        pltpu.make_async_copy(fresh, weights_out.at[tail], sem.at[2]),
    ]
    copies[0].start()
    copies[1].start()
    fresh[...] = weights[tail] - learn_rate * returned[waves - 1]
    copies[2].start()
    for copy in copies:
        copy.wait()


def solution(mesh):
    group = mesh.shape["fsdp"]

    def body(g, m, w):
        mats, near, wide = g.shape
        waves, side = mats // group, near * group
        f32 = jnp.float32
        block = jax.ShapeDtypeStruct(g.shape, f32)
        sem = pltpu.SemaphoreType.DMA
        in_hbm, in_vmem = pl.BlockSpec(memory_space=pltpu.HBM), pl.BlockSpec(memory_space=pltpu.VMEM)
        blocks = pltpu.VMEM((waves, group, near, wide), f32)
        split = jax.ShapeDtypeStruct(blocks.shape, f32)
        squares = pltpu.VMEM((waves, side, side), f32)
        weights, momentum, returned = pl.pallas_call(
            functools.partial(exchange, group, waves),
            name="update",
            out_shape=(block, block, split),
            in_specs=[in_hbm] * 3,
            out_specs=[in_vmem] * 3,
            scratch_shapes=[
                pltpu.VMEM(g.shape, f32),
                pltpu.VMEM(g.shape, f32),
                blocks,
                blocks,
                pltpu.VMEM((side, wide), f32),
                squares,
                squares,
                sem((2, waves)),
                sem,
                sem((waves,)),
                sem((waves,)),
                sem((waves,)),
                sem((waves,)),
                sem((waves,)),
                sem((waves,)),
                pltpu.SemaphoreType.REGULAR((group // 8,)),
                pltpu.SemaphoreType.REGULAR((group // 8 - 1,)),
                pltpu.SemaphoreType.REGULAR,
            ],
            compiler_params=pltpu.CompilerParams(
                collective_id=0, has_side_effects=True, vmem_limit_bytes=46 * MIB
            ),
        )(g, m, w)
        return pl.pallas_call(
            store,
            name="store",
            out_shape=(block, block),
            in_specs=[in_vmem] * 3,
            out_specs=[in_hbm] * 2,
            scratch_shapes=[pltpu.VMEM((group, near, wide), f32), sem((3,))],
            compiler_params=pltpu.CompilerParams(vmem_limit_bytes=16 * MIB),
        )(weights, momentum, returned)

    specs = P("shift", "fsdp", "tp")
    return jax.shard_map(
        body, mesh=mesh, in_specs=(specs,) * 3, out_specs=(specs,) * 2, check_vma=False
    )
```

```python
import functools

import jax
import jax.numpy as jnp
from jax import lax
from jax.experimental import pallas as pl
from jax.experimental.pallas import tpu as pltpu
from jax.sharding import PartitionSpec as P

MESH = pl.DeviceIdType.MESH
MIB = 1024 * 1024
ITERS = 3
hold_rate = 0.95
learn_rate = 0.9

CORNERS = ((1, 1), (0, 1), (1, 0), (0, 0))


def order():
    steps = [(dz, b, c) for dz in (5, 4, 3, 6, 2, 7, 1, 0) for b, c in CORNERS]
    return [step for step in steps if any(step)]


def full_dot(a, b, dims):
    return lax.dot_general(
        a, b, (dims, ((), ())), precision=lax.Precision.HIGHEST, preferred_element_type=jnp.float32
    )


def times(a, b):
    return full_dot(a, b, ((1,), (0,)))


def polynomial(gram):
    side = gram.shape[0]
    eye = lax.broadcasted_iota(jnp.int32, (side, side), 0) == lax.broadcasted_iota(
        jnp.int32, (side, side), 1
    )
    total = jnp.sum(jnp.sum(jnp.where(eye, gram, 0.0), axis=1, keepdims=True), axis=0, keepdims=True)
    scale = lax.rsqrt(total + 1e-06)
    a = gram * (scale * scale)
    whole = None
    for step in range(ITERS):
        mixed = -4.775 * a + 2.0315 * times(a, a)
        mixed = jnp.where(eye, mixed + 3.4445, mixed)
        whole = mixed if whole is None else times(mixed, whole)
        if step < ITERS - 1:
            a = times(times(mixed, a), mixed)
    return whole * scale


def exchange(
    group,
    waves,
    g_ref,
    m_ref,
    w_ref,
    weights,
    momentum,
    returned,
    g_buf,
    m_buf,
    arrived,
    leaving,
    rows,
    gram_out,
    gram_in,
    load_sem,
    w_sem,
    out_send,
    out_recv,
    gram_send,
    gram_recv,
    back_send,
    back_recv,
    up_sem,
    down_sem,
    side_sem,
):
    me, half = lax.axis_index("fsdp"), lax.axis_index("tp")
    near, other = rows.shape[0] // group, lax.rem(half + 1, 2)
    z, y, core = me // 4, lax.rem(me // 2, 2), lax.rem(me, 2)
    depth = group // 4

    def partner(step):
        dz, dy, dc = step
        turned = lax.rem(z, 2) * (depth - 2 * dz)
        return lax.rem(z + dz + turned, depth) * 4 + lax.rem(y + dy, 2) * 2 + lax.rem(core + dc, 2)

    def part(w):
        return pl.ds(w * group, group)

    barrier = pltpu.get_barrier_semaphore()

    def loads(w):
        return (
            pltpu.make_async_copy(g_ref.at[part(w)], g_buf.at[part(w)], load_sem.at[0, w]),
            pltpu.make_async_copy(m_ref.at[part(w)], m_buf.at[part(w)], load_sem.at[1, w]),
        )

    for copy in loads(0):
        copy.start()
    close = [s for s in order() if s[0] == 0 or s[0] in (1, depth - 1) and s[1] == 0]
    close.sort(key=lambda s: s[0] == 0)
    beside = {"fsdp": partner((0, 1, 0)), "tp": other}
    for step in close:
        pl.semaphore_signal(barrier, inc=1, device_id={"fsdp": partner(step)}, device_id_type=MESH)
    pl.semaphore_signal(barrier, inc=1, device_id=beside, device_id_type=MESH)
    for w in range(1, waves):
        for copy in loads(w):
            copy.start()

    def tell(sem, dz):
        to = lax.rem(me + 4 * dz, group)
        pl.semaphore_signal(sem, inc=1, device_id={"fsdp": to}, device_id_type=MESH)

    w_copy = pltpu.make_async_copy(w_ref, weights, w_sem)
    w_copy.start()

    def out_copy(w, to):
        return pltpu.make_async_remote_copy(
            src_ref=momentum.at[w * group + to],
            dst_ref=arrived.at[w, me],
            send_sem=out_send.at[w],
            recv_sem=out_recv.at[w],
            device_id={"fsdp": to},
            device_id_type=MESH,
        )

    def back_copy(w, to):
        return pltpu.make_async_remote_copy(
            src_ref=leaving.at[w, to],
            dst_ref=returned.at[w, me],
            send_sem=back_send.at[w],
            recv_sem=back_recv.at[w],
            device_id={"fsdp": to},
            device_id_type=MESH,
        )

    def all_of(buf, w, send, recv):
        blocks = buf.at[w, pl.ds(0, group - 1)]
        return pltpu.make_async_remote_copy(
            src_ref=blocks, dst_ref=blocks, send_sem=send.at[w], recv_sem=recv.at[w],
            device_id={"fsdp": me}, device_id_type=MESH,
        )

    def gram_copy(w):
        return pltpu.make_async_remote_copy(
            src_ref=gram_out.at[w],
            dst_ref=gram_in.at[w],
            send_sem=gram_send.at[w],
            recv_sem=gram_recv.at[w],
            device_id={"tp": other},
            device_id_type=MESH,
        )

    def momenta(w):
        for copy in loads(w):
            copy.wait()
        momentum[part(w)] = hold_rate * m_buf[part(w)] + g_buf[part(w)]
        arrived[w, me] = momentum[w * group + me]

    def first_out(hop):
        for dz, b, c in sorted(order(), key=lambda s: s[0] == 0):
            hops = min(dz, depth - dz)
            if hops == hop + 1 - b or hops == hop == 0:
                out_copy(0, partner((dz, b, c))).start()

    far = depth // 2
    momenta(0)
    pl.semaphore_wait(barrier, len(close) + 1)
    tell(up_sem.at[0], 1)
    tell(down_sem.at[0], depth - 1)
    first_out(0)
    pl.semaphore_signal(side_sem, inc=1, device_id=beside, device_id_type=MESH)
    for hop in range(1, far + 1):
        pl.semaphore_wait(up_sem.at[hop - 1], 1)
        if hop < far:
            tell(up_sem.at[hop], 1)
            pl.semaphore_wait(down_sem.at[hop - 1], 1)
            if hop < far - 1:
                tell(down_sem.at[hop], depth - 1)
        first_out(hop)
    for w in range(1, waves):
        momenta(w)
    pl.semaphore_wait(side_sem, 1)

    def send_out(w, _):
        for step in order():
            out_copy(w, partner(step)).start()
        return 0

    lax.fori_loop(1, waves, send_out, 0)

    def wave(w, _):
        all_of(arrived, w, out_send, out_recv).wait_recv()
        for k in range(group // 2):
            rows[pl.ds(2 * near * k, 2 * near), :] = jnp.concatenate(
                [arrived[w, 2 * k], arrived[w, 2 * k + 1]], axis=0
            )
        mat = rows[...]
        gram_out[w] = full_dot(mat, mat, ((1,), (1,)))
        gram_copy(w).start()
        gram_copy(w).wait_recv()
        mix = polynomial(gram_out[w] + gram_in[w])
        product = times(mix, rows[...])
        for k in range(group):
            leaving[w, k] = product[near * k : near * (k + 1)]
        @pl.when(w < waves - 1)
        def _():
            for step in order():
                back_copy(w, partner(step)).start()

        @pl.when(w >= waves - 1)
        def _():
            for to_z in (0, 1, 2, 3, 7, 4, 6, 5):
                for b, c in CORNERS:
                    to = to_z * 4 + lax.rem(y + b, 2) * 2 + lax.rem(core + c, 2)
                    if b or c:
                        back_copy(w, to).start()
                    else:
                        @pl.when(to != me)
                        def _(to=to):
                            back_copy(w, to).start()

        returned[w, me] = leaving[w, me]
        return 0

    lax.fori_loop(0, waves, wave, 0)
    w_copy.wait()

    def finish(w, _):
        all_of(returned, w, back_send, back_recv).wait_recv()
        weights[part(w)] = weights[part(w)] - learn_rate * returned[w]
        return 0

    lax.fori_loop(0, waves - 1, finish, 0)

    def drain(w, _):
        all_of(arrived, w, out_send, out_recv).wait_send()
        gram_copy(w).wait_send()
        all_of(returned, w, back_send, back_recv).wait_send()
        return 0

    lax.fori_loop(0, waves, drain, 0)
    all_of(returned, waves - 1, back_send, back_recv).wait_recv()


def is_early():
    return lax.axis_index("fsdp") < 12


def store_early(g_ref, m_ref, momentum_out, g_buf, m_buf, sem):
    @pl.when(is_early())
    def _():
        parts = [pl.ds(32 * i, 32) for i in range(g_buf.shape[0] // 32)]
        loads = [
            (
                pltpu.make_async_copy(g_ref.at[part], g_buf.at[part], sem.at[0, i]),
                pltpu.make_async_copy(m_ref.at[part], m_buf.at[part], sem.at[1, i]),
            )
            for i, part in enumerate(parts)
        ]
        stores = [
            pltpu.make_async_copy(g_buf.at[part], momentum_out.at[part], sem.at[2, i])
            for i, part in enumerate(parts)
        ]
        for pair in loads:
            for copy in pair:
                copy.start()
        for part, pair, copy in zip(parts, loads, stores):
            for load in pair:
                load.wait()
            g_buf[part] = hold_rate * m_buf[part] + g_buf[part]
            copy.start()
        for copy in stores:
            copy.wait()


def store(weights, momentum, returned, begun, weights_out, momentum_out, fresh, sem):
    waves, group = returned.shape[:2]
    done, tail = pl.ds(0, (waves - 1) * group), pl.ds((waves - 1) * group, group)
    copies = [
        pltpu.make_async_copy(weights.at[done], weights_out.at[done], sem.at[0]),
        pltpu.make_async_copy(fresh, weights_out.at[tail], sem.at[1]),
    ]
    other = pltpu.make_async_copy(momentum, momentum_out, sem.at[2])
    copies[0].start()

    @pl.when(jnp.logical_not(is_early()))
    def _():
        other.start()

    fresh[...] = weights[tail] - learn_rate * returned[waves - 1]
    copies[1].start()
    for copy in copies:
        copy.wait()

    @pl.when(jnp.logical_not(is_early()))
    def _():
        other.wait()


def solution(mesh):
    group = mesh.shape["fsdp"]

    def body(g, m, w):
        mats, near, wide = g.shape
        waves, side = mats // group, near * group
        f32 = jnp.float32
        block = jax.ShapeDtypeStruct(g.shape, f32)
        sem = pltpu.SemaphoreType.DMA
        in_hbm, in_vmem = pl.BlockSpec(memory_space=pltpu.HBM), pl.BlockSpec(memory_space=pltpu.VMEM)
        blocks = pltpu.VMEM((waves, group, near, wide), f32)
        split = jax.ShapeDtypeStruct(blocks.shape, f32)
        squares = pltpu.VMEM((waves, side, side), f32)
        begun = pl.pallas_call(
            store_early,
            name="store_early",
            out_shape=block,
            in_specs=[in_hbm] * 2,
            out_specs=in_hbm,
            scratch_shapes=[pltpu.VMEM(g.shape, f32), pltpu.VMEM(g.shape, f32), sem((3, mats // 32))],
            compiler_params=pltpu.CompilerParams(vmem_limit_bytes=60 * MIB, has_side_effects=True),
        )(g, m)
        weights, momentum, returned = pl.pallas_call(
            functools.partial(exchange, group, waves),
            name="update",
            out_shape=(block, block, split),
            in_specs=[in_hbm] * 3,
            out_specs=[in_vmem] * 3,
            scratch_shapes=[
                pltpu.VMEM(g.shape, f32),
                pltpu.VMEM(g.shape, f32),
                blocks,
                blocks,
                pltpu.VMEM((side, wide), f32),
                squares,
                squares,
                sem((2, waves)),
                sem,
                sem((waves,)),
                sem((waves,)),
                sem((waves,)),
                sem((waves,)),
                sem((waves,)),
                sem((waves,)),
                pltpu.SemaphoreType.REGULAR((group // 8,)),
                pltpu.SemaphoreType.REGULAR((group // 8 - 1,)),
                pltpu.SemaphoreType.REGULAR,
            ],
            compiler_params=pltpu.CompilerParams(
                collective_id=0, has_side_effects=True, vmem_limit_bytes=46 * MIB
            ),
        )(g, m, w)
        return pl.pallas_call(
            store,
            name="store",
            out_shape=(block, block),
            in_specs=[in_vmem] * 3 + [in_hbm],
            out_specs=[in_hbm] * 2,
            input_output_aliases={3: 1},
            scratch_shapes=[pltpu.VMEM((group, near, wide), f32), sem((3,))],
            compiler_params=pltpu.CompilerParams(vmem_limit_bytes=16 * MIB),
        )(weights, momentum, returned, begun)

    specs = P("shift", "fsdp", "tp")
    return jax.shard_map(
        body, mesh=mesh, in_specs=(specs,) * 3, out_specs=(specs,) * 2, check_vma=False
    )
```

```python
import functools

import jax
import jax.numpy as jnp
from jax import lax
from jax.experimental import pallas as pl
from jax.experimental.pallas import tpu as pltpu
from jax.sharding import PartitionSpec as P

MESH = pl.DeviceIdType.MESH
MIB = 1024 * 1024
ITERS = 3
hold_rate = 0.95
learn_rate = 0.9

CORNERS = ((1, 1), (0, 1), (1, 0), (0, 0))


def order():
    steps = [(dz, b, c) for dz in (5, 4, 3, 6, 2, 7, 1, 0) for b, c in CORNERS]
    return [step for step in steps if any(step)]


def full_dot(a, b, dims):
    return lax.dot_general(
        a, b, (dims, ((), ())), precision=lax.Precision.HIGHEST, preferred_element_type=jnp.float32
    )


def times(a, b):
    return full_dot(a, b, ((1,), (0,)))


def polynomial(gram):
    side = gram.shape[0]
    eye = lax.broadcasted_iota(jnp.int32, (side, side), 0) == lax.broadcasted_iota(
        jnp.int32, (side, side), 1
    )
    total = jnp.sum(jnp.sum(jnp.where(eye, gram, 0.0), axis=1, keepdims=True), axis=0, keepdims=True)
    scale = lax.rsqrt(total + 1e-06)
    a = gram * (scale * scale)
    whole = None
    for step in range(ITERS):
        mixed = -4.775 * a + 2.0315 * times(a, a)
        mixed = jnp.where(eye, mixed + 3.4445, mixed)
        whole = mixed if whole is None else times(mixed, whole)
        if step < ITERS - 1:
            a = times(times(mixed, a), mixed)
    return whole * scale


def exchange(
    group,
    waves,
    g_ref,
    m_ref,
    w_ref,
    weights,
    momentum,
    returned,
    g_buf,
    m_buf,
    arrived,
    leaving,
    rows,
    gram_out,
    gram_in,
    load_sem,
    w_sem,
    out_send,
    out_recv,
    gram_send,
    gram_recv,
    back_send,
    back_recv,
    up_sem,
    down_sem,
    side_sem,
):
    me, half = lax.axis_index("fsdp"), lax.axis_index("tp")
    near, other = rows.shape[0] // group, lax.rem(half + 1, 2)
    z, y, core = me // 4, lax.rem(me // 2, 2), lax.rem(me, 2)
    depth = group // 4

    def partner(step):
        dz, dy, dc = step
        turned = lax.rem(z, 2) * (depth - 2 * dz)
        return lax.rem(z + dz + turned, depth) * 4 + lax.rem(y + dy, 2) * 2 + lax.rem(core + dc, 2)

    def part(w):
        return pl.ds(w * group, group)

    barrier = pltpu.get_barrier_semaphore()

    def loads(w):
        return (
            pltpu.make_async_copy(g_ref.at[part(w)], g_buf.at[part(w)], load_sem.at[0, w]),
            pltpu.make_async_copy(m_ref.at[part(w)], m_buf.at[part(w)], load_sem.at[1, w]),
        )

    for copy in loads(0):
        copy.start()
    close = [s for s in order() if s[0] == 0 or s[0] in (1, depth - 1) and s[1] == 0]
    close.sort(key=lambda s: s[0] == 0)
    beside = {"fsdp": partner((0, 1, 0)), "tp": other}
    for step in close:
        pl.semaphore_signal(barrier, inc=1, device_id={"fsdp": partner(step)}, device_id_type=MESH)
    pl.semaphore_signal(barrier, inc=1, device_id=beside, device_id_type=MESH)
    def tell(sem, dz):
        to = lax.rem(me + 4 * dz, group)
        pl.semaphore_signal(sem, inc=1, device_id={"fsdp": to}, device_id_type=MESH)

    w_copy = pltpu.make_async_copy(w_ref, weights, w_sem)

    def out_copy(w, to):
        return pltpu.make_async_remote_copy(
            src_ref=momentum.at[w * group + to],
            dst_ref=arrived.at[w, me],
            send_sem=out_send.at[w],
            recv_sem=out_recv.at[w],
            device_id={"fsdp": to},
            device_id_type=MESH,
        )

    def back_copy(w, to):
        return pltpu.make_async_remote_copy(
            src_ref=leaving.at[w, to],
            dst_ref=returned.at[w, me],
            send_sem=back_send.at[w],
            recv_sem=back_recv.at[w],
            device_id={"fsdp": to},
            device_id_type=MESH,
        )

    def all_of(buf, w, send, recv):
        blocks = buf.at[w, pl.ds(0, group - 1)]
        return pltpu.make_async_remote_copy(
            src_ref=blocks, dst_ref=blocks, send_sem=send.at[w], recv_sem=recv.at[w],
            device_id={"fsdp": me}, device_id_type=MESH,
        )

    def gram_copy(w):
        return pltpu.make_async_remote_copy(
            src_ref=gram_out.at[w],
            dst_ref=gram_in.at[w],
            send_sem=gram_send.at[w],
            recv_sem=gram_recv.at[w],
            device_id={"tp": other},
            device_id_type=MESH,
        )

    def momenta(w):
        for copy in loads(w):
            copy.wait()
        if w == 0:
            for later in range(1, waves):
                for copy in loads(later):
                    copy.start()
        momentum[part(w)] = hold_rate * m_buf[part(w)] + g_buf[part(w)]
        arrived[w, me] = momentum[w * group + me]

    def first_out(hop):
        for dz, b, c in sorted(order(), key=lambda s: s[0] == 0):
            hops = min(dz, depth - dz)
            if hops == hop + 1 - b or hops == hop == 0:
                out_copy(0, partner((dz, b, c))).start()

    far = depth // 2
    momenta(0)
    pl.semaphore_wait(barrier, len(close) + 1)
    tell(up_sem.at[0], 1)
    tell(down_sem.at[0], depth - 1)
    first_out(0)
    pl.semaphore_signal(side_sem, inc=1, device_id=beside, device_id_type=MESH)
    for hop in range(1, far + 1):
        pl.semaphore_wait(up_sem.at[hop - 1], 1)
        if hop < far:
            tell(up_sem.at[hop], 1)
            pl.semaphore_wait(down_sem.at[hop - 1], 1)
            if hop < far - 1:
                tell(down_sem.at[hop], depth - 1)
        first_out(hop)
    for w in range(1, waves):
        momenta(w)
    pl.semaphore_wait(side_sem, 1)

    def send_out(w, _):
        for step in order():
            out_copy(w, partner(step)).start()
        return 0

    lax.fori_loop(1, waves, send_out, 0)
    w_copy.start()

    def wave(w, _):
        all_of(arrived, w, out_send, out_recv).wait_recv()
        for k in range(group // 2):
            rows[pl.ds(2 * near * k, 2 * near), :] = jnp.concatenate(
                [arrived[w, 2 * k], arrived[w, 2 * k + 1]], axis=0
            )
        mat = rows[...]
        gram_out[w] = full_dot(mat, mat, ((1,), (1,)))
        gram_copy(w).start()
        gram_copy(w).wait_recv()
        mix = polynomial(gram_out[w] + gram_in[w])
        product = times(mix, rows[...])
        for k in range(group):
            leaving[w, k] = product[near * k : near * (k + 1)]
        @pl.when(w < waves - 1)
        def _():
            for step in order():
                back_copy(w, partner(step)).start()

        @pl.when(w >= waves - 1)
        def _():
            for to_z in (0, 1, 2, 3, 7, 4, 6, 5):
                for b, c in CORNERS:
                    to = to_z * 4 + lax.rem(y + b, 2) * 2 + lax.rem(core + c, 2)
                    if b or c:
                        back_copy(w, to).start()
                    else:
                        @pl.when(to != me)
                        def _(to=to):
                            back_copy(w, to).start()

        returned[w, me] = leaving[w, me]
        return 0

    lax.fori_loop(0, waves, wave, 0)
    w_copy.wait()

    def finish(w, _):
        all_of(returned, w, back_send, back_recv).wait_recv()
        weights[part(w)] = weights[part(w)] - learn_rate * returned[w]
        return 0

    lax.fori_loop(0, waves - 1, finish, 0)

    def drain(w, _):
        all_of(arrived, w, out_send, out_recv).wait_send()
        gram_copy(w).wait_send()
        all_of(returned, w, back_send, back_recv).wait_send()
        return 0

    lax.fori_loop(0, waves, drain, 0)
    all_of(returned, waves - 1, back_send, back_recv).wait_recv()


def is_early():
    return lax.axis_index("fsdp") < 12


def store_early(g_ref, m_ref, momentum_out, g_buf, m_buf, sem):
    @pl.when(is_early())
    def _():
        parts = [pl.ds(32 * i, 32) for i in range(g_buf.shape[0] // 32)]
        loads = [
            (
                pltpu.make_async_copy(g_ref.at[part], g_buf.at[part], sem.at[0, i]),
                pltpu.make_async_copy(m_ref.at[part], m_buf.at[part], sem.at[1, i]),
            )
            for i, part in enumerate(parts)
        ]
        stores = [
            pltpu.make_async_copy(g_buf.at[part], momentum_out.at[part], sem.at[2, i])
            for i, part in enumerate(parts)
        ]
        for pair in loads:
            for copy in pair:
                copy.start()
        for part, pair, copy in zip(parts, loads, stores):
            for load in pair:
                load.wait()
            g_buf[part] = hold_rate * m_buf[part] + g_buf[part]
            copy.start()
        for copy in stores:
            copy.wait()


def store(weights, momentum, returned, begun, weights_out, momentum_out, fresh, sem):
    waves, group = returned.shape[:2]
    done, tail = pl.ds(0, (waves - 1) * group), pl.ds((waves - 1) * group, group)
    copies = [
        pltpu.make_async_copy(weights.at[done], weights_out.at[done], sem.at[0]),
        pltpu.make_async_copy(fresh, weights_out.at[tail], sem.at[1]),
    ]
    other = pltpu.make_async_copy(momentum, momentum_out, sem.at[2])
    copies[0].start()

    @pl.when(jnp.logical_not(is_early()))
    def _():
        other.start()

    fresh[...] = weights[tail] - learn_rate * returned[waves - 1]
    copies[1].start()
    for copy in copies:
        copy.wait()

    @pl.when(jnp.logical_not(is_early()))
    def _():
        other.wait()


def solution(mesh):
    group = mesh.shape["fsdp"]

    def body(g, m, w):
        mats, near, wide = g.shape
        waves, side = mats // group, near * group
        f32 = jnp.float32
        block = jax.ShapeDtypeStruct(g.shape, f32)
        sem = pltpu.SemaphoreType.DMA
        in_hbm, in_vmem = pl.BlockSpec(memory_space=pltpu.HBM), pl.BlockSpec(memory_space=pltpu.VMEM)
        blocks = pltpu.VMEM((waves, group, near, wide), f32)
        split = jax.ShapeDtypeStruct(blocks.shape, f32)
        squares = pltpu.VMEM((waves, side, side), f32)
        begun = pl.pallas_call(
            store_early,
            name="store_early",
            out_shape=block,
            in_specs=[in_hbm] * 2,
            out_specs=in_hbm,
            scratch_shapes=[pltpu.VMEM(g.shape, f32), pltpu.VMEM(g.shape, f32), sem((3, mats // 32))],
            compiler_params=pltpu.CompilerParams(vmem_limit_bytes=60 * MIB, has_side_effects=True),
        )(g, m)
        weights, momentum, returned = pl.pallas_call(
            functools.partial(exchange, group, waves),
            name="update",
            out_shape=(block, block, split),
            in_specs=[in_hbm] * 3,
            out_specs=[in_vmem] * 3,
            scratch_shapes=[
                pltpu.VMEM(g.shape, f32),
                pltpu.VMEM(g.shape, f32),
                blocks,
                blocks,
                pltpu.VMEM((side, wide), f32),
                squares,
                squares,
                sem((2, waves)),
                sem,
                sem((waves,)),
                sem((waves,)),
                sem((waves,)),
                sem((waves,)),
                sem((waves,)),
                sem((waves,)),
                pltpu.SemaphoreType.REGULAR((group // 8,)),
                pltpu.SemaphoreType.REGULAR((group // 8 - 1,)),
                pltpu.SemaphoreType.REGULAR,
            ],
            compiler_params=pltpu.CompilerParams(
                collective_id=0, has_side_effects=True, vmem_limit_bytes=46 * MIB
            ),
        )(g, m, w)
        return pl.pallas_call(
            store,
            name="store",
            out_shape=(block, block),
            in_specs=[in_vmem] * 3 + [in_hbm],
            out_specs=[in_hbm] * 2,
            input_output_aliases={3: 1},
            scratch_shapes=[pltpu.VMEM((group, near, wide), f32), sem((3,))],
            compiler_params=pltpu.CompilerParams(vmem_limit_bytes=16 * MIB),
        )(weights, momentum, returned, begun)

    specs = P("shift", "fsdp", "tp")
    return jax.shard_map(
        body, mesh=mesh, in_specs=(specs,) * 3, out_specs=(specs,) * 2, check_vma=False
    )
```

```python
import functools

import jax
import jax.numpy as jnp
from jax import lax
from jax.experimental import pallas as pl
from jax.experimental.pallas import tpu as pltpu
from jax.sharding import PartitionSpec as P

MESH = pl.DeviceIdType.MESH
MIB = 1024 * 1024
ITERS = 3
hold_rate = 0.95
learn_rate = 0.9

CORNERS = ((1, 1), (0, 1), (1, 0), (0, 0))


def order():
    steps = [(dz, b, c) for dz in (5, 4, 3, 6, 2, 7, 1, 0) for b, c in CORNERS]
    return [step for step in steps if any(step)]


def full_dot(a, b, dims):
    return lax.dot_general(
        a, b, (dims, ((), ())), precision=lax.Precision.HIGHEST, preferred_element_type=jnp.float32
    )


def times(a, b):
    return full_dot(a, b, ((1,), (0,)))


def polynomial(gram):
    side = gram.shape[0]
    eye = lax.broadcasted_iota(jnp.int32, (side, side), 0) == lax.broadcasted_iota(
        jnp.int32, (side, side), 1
    )
    total = jnp.sum(jnp.sum(jnp.where(eye, gram, 0.0), axis=1, keepdims=True), axis=0, keepdims=True)
    scale = lax.rsqrt(total + 1e-06)
    a = gram * (scale * scale)
    whole = None
    for step in range(ITERS):
        mixed = -4.775 * a + 2.0315 * times(a, a)
        mixed = jnp.where(eye, mixed + 3.4445, mixed)
        whole = mixed if whole is None else times(mixed, whole)
        if step < ITERS - 1:
            a = times(times(mixed, a), mixed)
    return whole * scale


def exchange(
    group,
    waves,
    g_ref,
    m_ref,
    w_ref,
    weights,
    momentum,
    returned,
    g_buf,
    m_buf,
    arrived,
    leaving,
    rows,
    gram_out,
    gram_in,
    load_sem,
    w_sem,
    out_send,
    out_recv,
    gram_send,
    gram_recv,
    back_send,
    back_recv,
    up_sem,
    down_sem,
    side_sem,
):
    me, half = lax.axis_index("fsdp"), lax.axis_index("tp")
    near, other = rows.shape[0] // group, lax.rem(half + 1, 2)
    z, y, core = me // 4, lax.rem(me // 2, 2), lax.rem(me, 2)
    depth = group // 4

    def partner(step):
        dz, dy, dc = step
        turned = lax.rem(z, 2) * (depth - 2 * dz)
        return lax.rem(z + dz + turned, depth) * 4 + lax.rem(y + dy, 2) * 2 + lax.rem(core + dc, 2)

    def part(w):
        return pl.ds(w * group, group)

    barrier = pltpu.get_barrier_semaphore()

    def loads(w):
        return (
            pltpu.make_async_copy(g_ref.at[part(w)], g_buf.at[part(w)], load_sem.at[0, w]),
            pltpu.make_async_copy(m_ref.at[part(w)], m_buf.at[part(w)], load_sem.at[1, w]),
        )

    for copy in loads(0):
        copy.start()
    close = [s for s in order() if s[0] == 0 or s[0] in (1, depth - 1) and s[1] == 0]
    close.sort(key=lambda s: s[0] == 0)
    beside = {"fsdp": partner((0, 1, 0)), "tp": other}
    for step in close:
        pl.semaphore_signal(barrier, inc=1, device_id={"fsdp": partner(step)}, device_id_type=MESH)
    pl.semaphore_signal(barrier, inc=1, device_id=beside, device_id_type=MESH)
    for w in range(1, waves):
        for copy in loads(w):
            copy.start()

    def tell(sem, dz):
        to = lax.rem(me + 4 * dz, group)
        pl.semaphore_signal(sem, inc=1, device_id={"fsdp": to}, device_id_type=MESH)

    w_copy = pltpu.make_async_copy(w_ref, weights, w_sem)
    w_copy.start()

    def out_copy(w, to):
        return pltpu.make_async_remote_copy(
            src_ref=momentum.at[w * group + to],
            dst_ref=arrived.at[w, me],
            send_sem=out_send.at[w],
            recv_sem=out_recv.at[w],
            device_id={"fsdp": to},
            device_id_type=MESH,
        )

    def back_copy(w, to):
        return pltpu.make_async_remote_copy(
            src_ref=leaving.at[w, to],
            dst_ref=returned.at[w, me],
            send_sem=back_send.at[w],
            recv_sem=back_recv.at[w],
            device_id={"fsdp": to},
            device_id_type=MESH,
        )

    def all_of(buf, w, send, recv):
        blocks = buf.at[w, pl.ds(0, group - 1)]
        return pltpu.make_async_remote_copy(
            src_ref=blocks, dst_ref=blocks, send_sem=send.at[w], recv_sem=recv.at[w],
            device_id={"fsdp": me}, device_id_type=MESH,
        )

    def gram_copy(w):
        return pltpu.make_async_remote_copy(
            src_ref=gram_out.at[w],
            dst_ref=gram_in.at[w],
            send_sem=gram_send.at[w],
            recv_sem=gram_recv.at[w],
            device_id={"tp": other},
            device_id_type=MESH,
        )

    def momenta(w):
        for copy in loads(w):
            copy.wait()
        momentum[part(w)] = hold_rate * m_buf[part(w)] + g_buf[part(w)]
        arrived[w, me] = momentum[w * group + me]

    def first_out(hop):
        for dz, b, c in sorted(order(), key=lambda s: s[0] == 0):
            hops = min(dz, depth - dz)
            if hops == hop + 1 - b or hops == hop == 0:
                out_copy(0, partner((dz, b, c))).start()

    far = depth // 2
    momenta(0)
    pl.semaphore_wait(barrier, len(close) + 1)
    tell(up_sem.at[0], 1)
    tell(down_sem.at[0], depth - 1)
    first_out(0)
    pl.semaphore_signal(side_sem, inc=1, device_id=beside, device_id_type=MESH)
    for hop in range(1, far + 1):
        pl.semaphore_wait(up_sem.at[hop - 1], 1)
        if hop < far:
            tell(up_sem.at[hop], 1)
            pl.semaphore_wait(down_sem.at[hop - 1], 1)
            if hop < far - 1:
                tell(down_sem.at[hop], depth - 1)
        first_out(hop)
    for w in range(1, waves):
        momenta(w)
    pl.semaphore_wait(side_sem, 1)

    def send_out(w, _):
        for step in order():
            out_copy(w, partner(step)).start()
        return 0

    lax.fori_loop(1, waves, send_out, 0)

    def wave(w, _):
        all_of(arrived, w, out_send, out_recv).wait_recv()
        for k in range(group // 2):
            rows[pl.ds(2 * near * k, 2 * near), :] = jnp.concatenate(
                [arrived[w, 2 * k], arrived[w, 2 * k + 1]], axis=0
            )
        mat = rows[...]
        gram_out[w] = full_dot(mat, mat, ((1,), (1,)))
        gram_copy(w).start()
        gram_copy(w).wait_recv()
        mix = polynomial(gram_out[w] + gram_in[w])
        product = times(mix, rows[...])
        for k in range(group):
            leaving[w, k] = product[near * k : near * (k + 1)]
        @pl.when(w < waves - 1)
        def _():
            for step in order():
                back_copy(w, partner(step)).start()

        @pl.when(w >= waves - 1)
        def _():
            for to_z in (0, 1, 2, 7, 3, 4, 6, 5):
                for b, c in CORNERS:
                    to = to_z * 4 + lax.rem(y + b, 2) * 2 + lax.rem(core + c, 2)
                    if b or c:
                        back_copy(w, to).start()
                    else:
                        @pl.when(to != me)
                        def _(to=to):
                            back_copy(w, to).start()

        returned[w, me] = leaving[w, me]
        return 0

    lax.fori_loop(0, waves, wave, 0)
    w_copy.wait()

    def finish(w, _):
        all_of(returned, w, back_send, back_recv).wait_recv()
        weights[part(w)] = weights[part(w)] - learn_rate * returned[w]
        return 0

    lax.fori_loop(0, waves - 1, finish, 0)

    def drain(w, _):
        all_of(arrived, w, out_send, out_recv).wait_send()
        gram_copy(w).wait_send()
        all_of(returned, w, back_send, back_recv).wait_send()
        return 0

    lax.fori_loop(0, waves, drain, 0)
    all_of(returned, waves - 1, back_send, back_recv).wait_recv()


def is_early():
    return lax.axis_index("fsdp") < 12


def store_early(g_ref, m_ref, momentum_out, g_buf, m_buf, sem):
    @pl.when(is_early())
    def _():
        parts = [pl.ds(32 * i, 32) for i in range(g_buf.shape[0] // 32)]
        loads = [
            (
                pltpu.make_async_copy(g_ref.at[part], g_buf.at[part], sem.at[0, i]),
                pltpu.make_async_copy(m_ref.at[part], m_buf.at[part], sem.at[1, i]),
            )
            for i, part in enumerate(parts)
        ]
        stores = [
            pltpu.make_async_copy(g_buf.at[part], momentum_out.at[part], sem.at[2, i])
            for i, part in enumerate(parts)
        ]
        for pair in loads:
            for copy in pair:
                copy.start()
        for part, pair, copy in zip(parts, loads, stores):
            for load in pair:
                load.wait()
            g_buf[part] = hold_rate * m_buf[part] + g_buf[part]
            copy.start()
        for copy in stores:
            copy.wait()


def store(weights, momentum, returned, begun, weights_out, momentum_out, fresh, sem):
    waves, group = returned.shape[:2]
    done, tail = pl.ds(0, (waves - 1) * group), pl.ds((waves - 1) * group, group)
    copies = [
        pltpu.make_async_copy(weights.at[done], weights_out.at[done], sem.at[0]),
        pltpu.make_async_copy(fresh, weights_out.at[tail], sem.at[1]),
    ]
    other = pltpu.make_async_copy(momentum, momentum_out, sem.at[2])
    copies[0].start()

    @pl.when(jnp.logical_not(is_early()))
    def _():
        other.start()

    fresh[...] = weights[tail] - learn_rate * returned[waves - 1]
    copies[1].start()
    for copy in copies:
        copy.wait()

    @pl.when(jnp.logical_not(is_early()))
    def _():
        other.wait()


def solution(mesh):
    group = mesh.shape["fsdp"]

    def body(g, m, w):
        mats, near, wide = g.shape
        waves, side = mats // group, near * group
        f32 = jnp.float32
        block = jax.ShapeDtypeStruct(g.shape, f32)
        sem = pltpu.SemaphoreType.DMA
        in_hbm, in_vmem = pl.BlockSpec(memory_space=pltpu.HBM), pl.BlockSpec(memory_space=pltpu.VMEM)
        blocks = pltpu.VMEM((waves, group, near, wide), f32)
        split = jax.ShapeDtypeStruct(blocks.shape, f32)
        squares = pltpu.VMEM((waves, side, side), f32)
        begun = pl.pallas_call(
            store_early,
            name="store_early",
            out_shape=block,
            in_specs=[in_hbm] * 2,
            out_specs=in_hbm,
            scratch_shapes=[pltpu.VMEM(g.shape, f32), pltpu.VMEM(g.shape, f32), sem((3, mats // 32))],
            compiler_params=pltpu.CompilerParams(vmem_limit_bytes=60 * MIB, has_side_effects=True),
        )(g, m)
        weights, momentum, returned = pl.pallas_call(
            functools.partial(exchange, group, waves),
            name="update",
            out_shape=(block, block, split),
            in_specs=[in_hbm] * 3,
            out_specs=[in_vmem] * 3,
            scratch_shapes=[
                pltpu.VMEM(g.shape, f32),
                pltpu.VMEM(g.shape, f32),
                blocks,
                blocks,
                pltpu.VMEM((side, wide), f32),
                squares,
                squares,
                sem((2, waves)),
                sem,
                sem((waves,)),
                sem((waves,)),
                sem((waves,)),
                sem((waves,)),
                sem((waves,)),
                sem((waves,)),
                pltpu.SemaphoreType.REGULAR((group // 8,)),
                pltpu.SemaphoreType.REGULAR((group // 8 - 1,)),
                pltpu.SemaphoreType.REGULAR,
            ],
            compiler_params=pltpu.CompilerParams(
                collective_id=0, has_side_effects=True, vmem_limit_bytes=46 * MIB
            ),
        )(g, m, w)
        return pl.pallas_call(
            store,
            name="store",
            out_shape=(block, block),
            in_specs=[in_vmem] * 3 + [in_hbm],
            out_specs=[in_hbm] * 2,
            input_output_aliases={3: 1},
            scratch_shapes=[pltpu.VMEM((group, near, wide), f32), sem((3,))],
            compiler_params=pltpu.CompilerParams(vmem_limit_bytes=16 * MIB),
        )(weights, momentum, returned, begun)

    specs = P("shift", "fsdp", "tp")
    return jax.shard_map(
        body, mesh=mesh, in_specs=(specs,) * 3, out_specs=(specs,) * 2, check_vma=False
    )
```
